32 devices in a mesh: shard: 4 (over y, x), tp: 8 (over z, core).
Axes of the slice: x: 2, y: 2, z: 4, core: 2. Of those that a mesh axis runs over, the one named last changes fastest.
Arguments:
- w_gate: float32 [5120, 17408], P('shard', 'tp'), may hold values from -0.125 to 0.125
- first_gate: float32 [5120, 17408], P('shard', 'tp'), may hold values from -0.078125 to 0.078125
- second_gate: float32 [5120, 17408], P('shard', 'tp'), may hold values from -0.078125 to 0.078125
- w_up: float32 [5120, 17408], P('shard', 'tp'), may hold values from -0.125 to 0.125
- first_up: float32 [5120, 17408], P('shard', 'tp'), may hold values from -0.078125 to 0.078125
- second_up: float32 [5120, 17408], P('shard', 'tp'), may hold values from -0.078125 to 0.078125
- norm_gain: float32 [5120], P('shard'), may hold values from 0.25 to 1.75
Outputs:
- serving_gate: bfloat16 [5120, 17408], P(None, 'tp')
- serving_up: bfloat16 [5120, 17408], P(None, 'tp')
- column_gate: float32 [17408], P('tp')
- column_up: float32 [17408], P('tp')
The draws below stay inside these ranges and needn't reach their ends.
All inputs are finite; a program needn't handle non-finite values.
Results may differ from the reference program's by a relative error of at most 0.001.
Values may be sent and summed in bfloat16 or wider, within the bound.
A program may use at most 256 MiB of HBM per device.

```python
import jax
import jax.numpy as jnp
from jax import lax

D_MODEL = 5120
D_INNER = 17408


def raised(array, rng, source, target, parts, factor):
    owner, partner = [(jnp.arange(array.shape[position]) // (array.shape[position] // parts)).reshape([-1 if axis == position else 1 for axis in range(array.ndim)]) for position in (source, target)]
    chosen = jax.random.permutation(rng, parts)[partner]
    strong = (owner == chosen) | (owner == (partner + parts // 2) % parts)
    return jnp.where(strong, factor * array, array)


def steps_of(key, extent, pieces, smallest, largest):
    def one(dim, shards_of):
        draws = jax.random.uniform(jax.random.fold_in(jax.random.fold_in(key, 6), dim), (shards_of,), jnp.float32, smallest / len(pieces), largest / len(pieces))
        return jnp.repeat(jnp.exp(draws), extent[dim] // shards_of).reshape((-1,) + (1,) * (len(extent) - dim - 1))

    loudness = one(*pieces[0])
    for cut in pieces[1:]:
        loudness = loudness * one(*cut)
    return loudness


def normal_values(own_key, extent, spread, reach, pieces=(), dtype=jnp.bfloat16):
    drawn = spread * jax.random.normal(own_key, extent, jnp.float32)
    if pieces:
        drawn = drawn * steps_of(own_key, extent, pieces, -0.22, 0.18)
    return jnp.clip(drawn, -reach, reach).astype(dtype)


def noise_with(own_key, shape, scale, most, split, heavy, dtype=jnp.bfloat16):
    values = scale * jax.random.normal(own_key, shape, jnp.float32)
    if split:
        values = values * steps_of(own_key, shape, split, -0.22, 0.18)
    return jnp.clip(raised(values, jax.random.fold_in(own_key, 3), *heavy), -most, most).astype(dtype)


def setup_inputs(seed: int = 0) -> dict:
    streams_of = jax.random.split(jax.random.key(seed), 8)
    w_gate = noise_with(streams_of[0], (D_MODEL, D_INNER), D_MODEL ** -0.5, 0.125, ((0, 4), (1, 8)), (0, 1, 8, 2.0), jnp.float32)
    first_gate = normal_values(streams_of[1], (D_MODEL, D_INNER), D_MODEL ** -0.5, 0.078125, ((0, 4), (1, 8)), jnp.float32)
    second_gate = normal_values(streams_of[2], (D_MODEL, D_INNER), D_MODEL ** -0.5, 0.078125, ((0, 4), (1, 8)), jnp.float32)
    w_up = noise_with(streams_of[3], (D_MODEL, D_INNER), D_MODEL ** -0.5, 0.125, ((0, 4), (1, 8)), (0, 1, 8, 2.0), jnp.float32)
    first_up = normal_values(streams_of[4], (D_MODEL, D_INNER), D_MODEL ** -0.5, 0.078125, ((0, 4), (1, 8)), jnp.float32)
    second_up = normal_values(streams_of[5], (D_MODEL, D_INNER), D_MODEL ** -0.5, 0.078125, ((0, 4), (1, 8)), jnp.float32)
    norm_gain = jnp.clip(1.0 + 0.15 * jax.random.normal(streams_of[6], (D_MODEL,), jnp.float32), 0.25, 1.75)
    return {"w_gate": w_gate, "first_gate": first_gate, "second_gate": second_gate, "w_up": w_up, "first_up": first_up, "second_up": second_up, "norm_gain": norm_gain}


learn_rate = 0.2
hold_rate = 0.8

def reference(w_gate, first_gate, second_gate, w_up, first_up, second_up, norm_gain):
    hold_gate = hold_rate * first_gate + second_gate
    whole_gate = w_gate - learn_rate * hold_gate
    hold_up = hold_rate * first_up + second_up
    whole_up = w_up - learn_rate * hold_up
    whole_gained_gate = whole_gate * norm_gain[:, None]
    whole_gained_up = whole_up * norm_gain[:, None]
    column_gate = jnp.sqrt(lax.optimization_barrier(jnp.sum(whole_gained_gate * whole_gained_gate, axis=0)))
    serving_gate = (whole_gained_gate / column_gate).astype(jnp.bfloat16)
    column_up = jnp.sqrt(lax.optimization_barrier(jnp.sum(whole_gained_up * whole_gained_up, axis=0)))
    serving_up = (whole_gained_up / column_up).astype(jnp.bfloat16)
    return (serving_gate, serving_up, column_gate, column_up)
```

```python
import functools

import jax
import jax.numpy as jnp
from jax import lax
from jax.experimental import pallas as pl
from jax.experimental.pallas import tpu as pltpu
from jax.sharding import PartitionSpec as P

learn_rate = 0.2
hold_rate = 0.8

LANES = 128
STEP = 32
MESH = pl.DeviceIdType.MESH


def plain(w_gate, first_gate, second_gate, w_up, first_up, second_up, norm_gain):
    hold_gate = hold_rate * first_gate + second_gate
    whole_gate = w_gate - learn_rate * hold_gate
    hold_up = hold_rate * first_up + second_up
    whole_up = w_up - learn_rate * hold_up
    whole_gained_gate = whole_gate * norm_gain[:, None]
    whole_gained_up = whole_up * norm_gain[:, None]
    total_gate, total_up = lax.psum(
        (
            jnp.sum(whole_gained_gate * whole_gained_gate, axis=0),
            jnp.sum(whole_gained_up * whole_gained_up, axis=0),
        ),
        "shard",
    )
    column_gate = jnp.sqrt(total_gate)
    column_up = jnp.sqrt(total_up)
    serving_gate, serving_up = (
        lax.all_gather((whole_gained_gate / column_gate).astype(jnp.bfloat16), "shard", axis=0, tiled=True),
        lax.all_gather((whole_gained_up / column_up).astype(jnp.bfloat16), "shard", axis=0, tiled=True),
    )
    return (serving_gate, serving_up, column_gate, column_up)


def cut(width, starts, most):
    tiles, sizes = width // LANES, []
    for size in starts:
        if tiles > size:
            sizes.append(size)
            tiles -= size
    while tiles > 0:
        sizes.append(min(most, tiles))
        tiles -= sizes[-1]
    chunks, at = [], 0
    for size in sizes:
        chunks.append((at * LANES, size * LANES))
        at += size
    return chunks


def kernel(
    chunks,
    rows,
    width,
    w_gate,
    first_gate,
    second_gate,
    w_up,
    first_up,
    second_up,
    gain,
    out_gate,
    out_up,
    columns,
    held,
    narrow,
    sums,
    load_sem,
    sum_send,
    sum_recv,
    own_send,
    own_recv,
    pass_send,
    pass_recv,
    local_sem,
):
    me = lax.axis_index("shard")
    row, column = me // 2, me % 2
    beside = row * 2 + (1 - column)
    above = (1 - row) * 2 + column
    across = (1 - row) * 2 + (1 - column)
    sources = ((w_gate, first_gate, second_gate), (w_up, first_up, second_up))
    outs = (out_gate, out_up)
    half = rows // 2

    def loads(k):
        which, first, size = chunks[k]
        return [
            pltpu.make_async_copy(
                ref.at[:, pl.ds(first, size)],
                held.at[k % 2, i, :, pl.ds(0, size)],
                load_sem.at[k % 2, i],
            )
            for i, ref in enumerate(sources[which])
        ]

    def send_sums(k):
        which, first, size = chunks[k]
        part = sums.at[me, :, pl.ds(which * width + first, size)]
        return [
            pltpu.make_async_remote_copy(
                src_ref=part,
                dst_ref=part,
                send_sem=sum_send.at[k, j],
                recv_sem=sum_recv.at[k, j],
                device_id={"shard": to},
                device_id_type=MESH,
            )
            for j, to in enumerate((beside, above, across))
        ]

    def send_own(k):
        which, first, size = chunks[k]
        return [
            pltpu.make_async_remote_copy(
                src_ref=narrow.at[:, pl.ds(which * width + first, size)],
                dst_ref=outs[which].at[pl.ds(me * rows, rows), pl.ds(first, size)],
                send_sem=own_send.at[k, j],
                recv_sem=own_recv.at[k, j],
                device_id={"shard": to},
                device_id_type=MESH,
            )
            for j, to in enumerate((beside, above))
        ]

    def keep_own(k):
        which, first, size = chunks[k]
        return pltpu.make_async_copy(
            narrow.at[:, pl.ds(which * width + first, size)],
            outs[which].at[pl.ds(me * rows, rows), pl.ds(first, size)],
            local_sem.at[k],
        )

    def send_on(k):
        which, first, size = chunks[k]
        copies = []
        for j, (origin, to) in enumerate(((above, beside), (beside, above))):
            part = outs[which].at[pl.ds(origin * rows + j * half, half), pl.ds(first, size)]
            copies.append(
                pltpu.make_async_remote_copy(
                    src_ref=part,
                    dst_ref=part,
                    send_sem=pass_send.at[k, j],
                    recv_sem=pass_recv.at[k, j],
                    device_id={"shard": to},
                    device_id_type=MESH,
                )
            )
        return copies

    for k in range(min(2, len(chunks))):
        for copy in loads(k):
            copy.start()
    barrier = pltpu.get_barrier_semaphore()
    for peer in (beside, above, across):
        pl.semaphore_signal(barrier, inc=1, device_id={"shard": peer}, device_id_type=MESH)

    for k, (which, first, size) in enumerate(chunks):
        slot, tiles = k % 2, size // LANES
        for copy in loads(k):
            copy.wait()

        def add_up(step, totals):
            here = pl.ds(pl.multiple_of(step * STEP, STEP), STEP)
            scale = gain[here, :]
            new = []
            for t in range(tiles):
                lanes = pl.ds(t * LANES, LANES)
                hold = hold_rate * held[slot, 1, here, lanes] + held[slot, 2, here, lanes]
                value = (held[slot, 0, here, lanes] - learn_rate * hold) * scale
                held[slot, 0, here, lanes] = value
                new.append(totals[t] + jnp.sum((value * value).reshape(STEP // 8, 8, LANES), axis=0))
            return tuple(new)

        totals = lax.fori_loop(
            0, rows // STEP, add_up, tuple(jnp.zeros((8, LANES), jnp.float32) for _ in range(tiles))
        )
        for t in range(tiles):
            sums[me, :, pl.ds(which * width + first + t * LANES, LANES)] = totals[t]
        if k == 0:
            pl.semaphore_wait(barrier, 3)
        exchange = send_sums(k)
        for copy in exchange:
            copy.start()
        for copy in exchange:
            copy.wait_recv()
        place = pl.ds(which * width + first, size)
        total = (sums[0, :, place] + sums[1, :, place]) + (sums[2, :, place] + sums[3, :, place])
        scale_of = jnp.sqrt(jnp.sum(total, axis=0, keepdims=True))
        columns[which : which + 1, pl.ds(first, size)] = scale_of
        inverse = 1.0 / scale_of

        def narrow_down(step, carry):
            here = pl.ds(pl.multiple_of(step * STEP, STEP), STEP)
            for t in range(tiles):
                value = held[slot, 0, here, pl.ds(t * LANES, LANES)]
                factor = inverse[:, t * LANES : (t + 1) * LANES]
                narrow[here, pl.ds(which * width + first + t * LANES, LANES)] = (value * factor).astype(jnp.bfloat16)
            return carry

        lax.fori_loop(0, rows // STEP, narrow_down, 0)
        for copy in send_own(k):
            copy.start()
        keep_own(k).start()
        if k + 2 < len(chunks):
            for copy in loads(k + 2):
                copy.start()

    for k in range(len(chunks)):
        arrived = send_own(k)
        onward = send_on(k)
        arrived[1].wait_recv()
        onward[0].start()
        arrived[0].wait_recv()
        onward[1].start()

    for k in range(len(chunks)):
        for copy in send_sums(k):
            copy.wait_send()
        for copy in send_own(k):
            copy.wait_send()
        keep_own(k).wait()
        for copy in send_on(k):
            copy.wait()


def per_device(w_gate, first_gate, second_gate, w_up, first_up, second_up, norm_gain):
    rows, width = w_gate.shape
    shards = lax.axis_size("shard")
    if shards != 4 or width % LANES or rows % (2 * STEP):
        return plain(w_gate, first_gate, second_gate, w_up, first_up, second_up, norm_gain)
    chunks = [(0, *chunk) for chunk in cut(width, (1, 2), 4)] + [(1, *chunk) for chunk in cut(width, (), 4)]
    most = max(size for _, _, size in chunks)
    count = len(chunks)
    gain = jnp.broadcast_to(norm_gain[:, None], (rows, LANES))
    anywhere = pl.BlockSpec(memory_space=pl.ANY)
    in_vmem = pl.BlockSpec(memory_space=pltpu.VMEM)
    dma = pltpu.SemaphoreType.DMA
    serving_gate, serving_up, columns = pl.pallas_call(
        functools.partial(kernel, chunks, rows, width),
        out_shape=(
            jax.ShapeDtypeStruct((shards * rows, width), jnp.bfloat16),
            jax.ShapeDtypeStruct((shards * rows, width), jnp.bfloat16),
            jax.ShapeDtypeStruct((2, width), jnp.float32),
        ),
        in_specs=[anywhere] * 6 + [in_vmem],
        out_specs=(anywhere, anywhere, in_vmem),
        scratch_shapes=[
            pltpu.VMEM((2, 3, rows, most), jnp.float32),
            pltpu.VMEM((rows, 2 * width), jnp.bfloat16),
            pltpu.VMEM((4, 8, 2 * width), jnp.float32),
            dma((2, 3)),
            dma((count, 3)),
            dma((count, 3)),
            dma((count, 2)),
            dma((count, 2)),
            dma((count, 2)),
            dma((count, 2)),
            dma((count,)),
        ],
        compiler_params=pltpu.CompilerParams(
            collective_id=0, has_side_effects=True, vmem_limit_bytes=48 * 1024 * 1024
        ),
    )(w_gate, first_gate, second_gate, w_up, first_up, second_up, gain)
    return (serving_gate, serving_up, columns[0], columns[1])


def solution(mesh):
    return jax.shard_map(
        per_device,
        mesh=mesh,
        in_specs=(
            P("shard", "tp"),
            P("shard", "tp"),
            P("shard", "tp"),
            P("shard", "tp"),
            P("shard", "tp"),
            P("shard", "tp"),
            P("shard"),
        ),
        out_specs=(P(None, "tp"), P(None, "tp"), P("tp"), P("tp")),
        check_vma=False,
    )
```
